32 devices in a mesh: grp: 8 (over y, x, core), own: 4 (over z).
Axes of the slice: x: 2, y: 2, z: 4, core: 2. Of those that a mesh axis runs over, the one named last changes fastest.
Arguments:
- background: bfloat16 [64, 1024, 512], P('grp', 'own'), may hold values from -6 to 6
- obs_ens: bfloat16 [64, 2048, 512], P('grp', 'own'), may hold values from -12 to 12
- innovation: bfloat16 [64, 2048], P('grp', 'own'), may hold values from -6 to 6
- obs_weight: bfloat16 [64, 2048], P('grp', 'own'), may hold values from 0.25 to 4
- obs_count: int32 [64, 4], P('grp', 'own'), may hold values from 128 to 512, as said below
- dest: int32 [64], replicated, may hold values from 0 to 7, as said below
Outputs:
- analysis: bfloat16 [64, 1024, 512], P('grp', 'own')
The draws below stay inside these ranges and needn't reach their ends.
Inputs may be any that keep to these rules, and one draw needn't show every extreme that they name: `obs_count`: each entry counts the live leading slots of one owner's block of 512; later slots carry values that must be ignored. The largest entry of every draw equals 512. `dest`: every index of grp is named by exactly 8 groups, and no two groups of one index of grp name the same index.
All inputs are finite; a program needn't handle non-finite values.
Results may differ from the reference program's by a relative error of at most 0.012.
The reference program's roundings to bfloat16 on the way (of `obs_pert`, `weight`, `source`, `weighted`, `inverse`, `weights`, `state_pert` and `result`) count: a program that leaves them out, or rounds other values in their place, can miss the bound.
Values may be sent and summed in bfloat16 or wider, within the bound.
No kernel may reach another device: no remote copies, remote signals or barrier semaphores. Data moves between devices by JAX's collectives and lax.ppermute only.
A program may use at most 128 MiB of HBM per device.

```python
import math
import jax
import jax.numpy as jnp
from jax import lax

MEMBERS = 512
G_DEV = 8
OBS_OWN = 512
NS_IT = 4
ROWS = 1024
OBS = 2048
GROUPS = 64


def draw_obs_ens(key, part):
    subkeys = jax.random.split(key, 2)
    row_scale = jnp.exp(jax.random.uniform(subkeys[0], (GROUPS, OBS, 1), minval=math.log(0.3), maxval=math.log(3.0)))
    values = jax.random.normal(subkeys[1], (GROUPS, OBS, MEMBERS)) * row_scale
    return jnp.clip(values, -12.0, 12.0).astype(jnp.bfloat16)


def draw_obs_count(key, part):
    subkeys = jax.random.split(key, 4)
    host_total = GROUPS // G_DEV
    owners = OBS // OBS_OWN
    floor_count = OBS_OWN // 4
    density = jax.random.randint(subkeys[0], (host_total,), 1, 9)
    density = density.at[jax.random.randint(subkeys[1], (), 0, host_total)].set(8)
    ceiling = floor_count + density * (OBS_OWN - floor_count) // 8
    ceiling_rows = jnp.repeat(ceiling, G_DEV)[:, None]
    counts = jax.random.randint(subkeys[2], (GROUPS, owners), floor_count, ceiling_rows + 1)
    chosen = jax.random.randint(subkeys[3], (), 0, GROUPS * owners)
    flattened = counts.reshape(-1).at[chosen].set(OBS_OWN)
    return flattened.reshape(GROUPS, owners).astype(jnp.int32)


def draw_dest(key, part):
    subkeys = jax.random.split(key, 2)
    host_total = GROUPS // G_DEV
    shuffle = jax.random.permutation(subkeys[0], host_total)
    offsets = jax.random.permutation(subkeys[1], host_total)[:G_DEV]
    target = (shuffle[:, None] + offsets[None, :]) % host_total
    return target.reshape(GROUPS).astype(jnp.int32)


def block_scale(stream_key, dims, pieces, least, top_value):
    loudness = 1.0
    for dim, parts in pieces:
        draws = jax.random.uniform(jax.random.fold_in(jax.random.fold_in(stream_key, 6), dim), (parts,), jnp.float32, least / len(pieces), top_value / len(pieces))
        loudness = loudness * jnp.repeat(jnp.exp(draws), dims[dim] // parts).reshape((-1,) + (1,) * (len(dims) - 1 - dim))
    return loudness


def noise(stream_key, extent, spread, reach, shards=(), kind=jnp.bfloat16):
    gain = block_scale(stream_key, extent, shards, -0.22, 0.18) if shards else 1.0
    values = jax.random.normal(stream_key, extent, jnp.float32) * spread * gain
    return jnp.minimum(jnp.maximum(values, -reach), reach).astype(kind)


def setup_inputs(seed: int = 0) -> dict:
    seeds = jax.random.split(jax.random.key(seed), 7)
    background = noise(seeds[0], (GROUPS, ROWS, MEMBERS), 1.0, 6.0, ((0, 8), (1, 4)))
    obs_ens = draw_obs_ens(jax.random.fold_in(seeds[6], 71), 0)
    innovation = noise(seeds[2], (GROUPS, OBS), 1.0, 6.0, ((0, 8), (1, 4)))
    obs_weight = jnp.clip(jnp.exp(math.log(4.0) - 2.7725887 * jax.random.uniform(seeds[3], (GROUPS, OBS), jnp.float32) ** block_scale(seeds[3], (GROUPS, OBS), ((0, 8), (1, 4)), -0.2, 0.2)), 0.25, 4.0).astype(jnp.bfloat16)
    obs_count = draw_obs_count(jax.random.fold_in(seeds[6], 71), 0)
    dest = draw_dest(jax.random.fold_in(seeds[6], 71), 0)
    return dict(background=background, obs_ens=obs_ens, innovation=innovation, obs_weight=obs_weight, obs_count=obs_count, dest=dest)


def newton_weights(gram, right_side):
    eye_mat = jnp.eye(MEMBERS, dtype=jnp.float32)
    matrix = gram + (MEMBERS - 1.0) * eye_mat
    norm_scale = jnp.sqrt(jnp.sum(matrix * matrix))
    root_iter = (matrix / norm_scale).astype(jnp.bfloat16)
    inverse = eye_mat.astype(jnp.bfloat16)
    for iteration in range(NS_IT):
        product = jnp.dot(inverse, root_iter, preferred_element_type=jnp.float32)
        factor = (1.5 * eye_mat - 0.5 * product).astype(jnp.bfloat16)
        root_iter = jnp.dot(root_iter, factor, preferred_element_type=jnp.float32).astype(jnp.bfloat16)
        inverse = jnp.dot(factor, inverse, preferred_element_type=jnp.float32).astype(jnp.bfloat16)
    inverse_wide = inverse.astype(jnp.float32)
    half_way = jnp.dot(inverse_wide, right_side, precision=lax.Precision.HIGHEST)
    mean_weight = jnp.dot(inverse_wide, half_way, precision=lax.Precision.HIGHEST) / norm_scale
    weights = jnp.sqrt((MEMBERS - 1.0) / norm_scale) * inverse_wide + mean_weight[:, None]
    return weights.astype(jnp.bfloat16)

def analyse(items):
    background, obs_ens, innovation, obs_weight, counts = items
    obs_mean = lax.optimization_barrier(jnp.mean(obs_ens.astype(jnp.float32), axis=1, keepdims=True))
    obs_pert = (obs_ens.astype(jnp.float32) - obs_mean).astype(jnp.bfloat16)
    position_in = jnp.arange(OBS) % OBS_OWN
    live_rows = position_in < jnp.repeat(counts, OBS_OWN)
    weight = jnp.where(live_rows, obs_weight, jnp.zeros_like(obs_weight)).astype(jnp.bfloat16)
    source = (weight.astype(jnp.float32) * innovation.astype(jnp.float32)).astype(jnp.bfloat16)
    weighted = (obs_pert.astype(jnp.float32) * weight.astype(jnp.float32)[:, None]).astype(jnp.bfloat16)
    gram = jnp.dot(weighted.T, obs_pert, preferred_element_type=jnp.float32)
    right_side = jnp.dot(source, obs_pert, preferred_element_type=jnp.float32)
    weights = newton_weights(gram, right_side)
    state_mean = lax.optimization_barrier(jnp.mean(background.astype(jnp.float32), axis=1, keepdims=True))
    state_pert = (background.astype(jnp.float32) - state_mean).astype(jnp.bfloat16)
    result = state_mean + jnp.dot(state_pert, weights, preferred_element_type=jnp.float32)
    return result.astype(jnp.bfloat16)

def reference(background, obs_ens, innovation, obs_weight, obs_count, dest):
    results = lax.map(analyse, (background, obs_ens, innovation, obs_weight, obs_count))
    group_ids = jnp.arange(GROUPS).astype(jnp.int32)
    same_dest = dest[None, :] == dest[:, None]
    earlier = group_ids[None, :] < group_ids[:, None]
    arrival_rank = lax.optimization_barrier(jnp.sum(jnp.where(same_dest & earlier, 1, 0), axis=1)).astype(jnp.int32)
    slot_of = (dest * G_DEV + arrival_rank).astype(jnp.int32)
    holder = lax.optimization_barrier(jnp.sum(jnp.where(slot_of[None, :] == group_ids[:, None], group_ids[None, :], 0), axis=1)).astype(jnp.int32)
    return results[holder]
```

```python
import functools

import jax
import jax.numpy as jnp
from jax import lax
from jax.experimental import pallas as pl
from jax.experimental.pallas import tpu as pltpu
from jax.sharding import PartitionSpec as P

NS_IT = 4
LANES = 128
EXTRA = 16
F32 = jnp.float32
BF16 = jnp.bfloat16


def block_pairs(blocks):
    return [(i, j) for i in range(blocks) for j in range(i + 1, blocks)]


def packed_rows(members):
    blocks = members // LANES
    return (len(block_pairs(blocks)) + blocks // 2) * LANES + EXTRA


def square_iota():
    row = lax.broadcasted_iota(jnp.int32, (LANES, LANES), 0)
    col = lax.broadcasted_iota(jnp.int32, (LANES, LANES), 1)
    return row, col


def gram_kernel(offset, order_ref, count_ref, obs_ref, weight_ref, innov_ref, out_ref):
    group = order_ref[offset + pl.program_id(0)]
    slots, members = obs_ref.shape[1:]
    blocks = members // LANES
    obs = obs_ref[0].astype(F32)
    mean = jnp.mean(obs, axis=1, keepdims=True)
    pert = (obs - mean).astype(BF16)

    def own_row(ref):
        rows = lax.broadcasted_iota(jnp.int32, ref.shape, 0)
        return jnp.sum(jnp.where(rows == group, ref[...].astype(F32), 0.0), axis=0, keepdims=True)

    live = lax.broadcasted_iota(jnp.int32, (1, slots), 1) < count_ref[group]
    weight = jnp.where(live, own_row(weight_ref), 0.0)
    source = (weight * own_row(innov_ref)).astype(BF16)
    column = jnp.transpose(jnp.broadcast_to(weight, (LANES, slots)))
    column = jnp.concatenate([column] * blocks, axis=1)
    weighted = (pert.astype(F32) * column).astype(BF16)

    rhs = jnp.dot(jnp.broadcast_to(source, (16, slots)), pert, preferred_element_type=F32)[:8]
    parts = {}
    for i in range(0, blocks, 2):
        strip = lax.dot_general(
            weighted[:, i * LANES:(i + 2) * LANES], pert[:, i * LANES:],
            (((0,), (0,)), ((), ())), preferred_element_type=F32)
        for a in range(2):
            for j in range(i + a, blocks):
                parts[i + a, j] = strip[a * LANES:(a + 1) * LANES, (j - i) * LANES:(j - i + 1) * LANES]
    row, col = square_iota()
    at = 0
    for i, j in block_pairs(blocks):
        out_ref[0, at:at + LANES] = parts[i, j].astype(BF16)
        at += LANES
    sub = lax.broadcasted_iota(jnp.int32, (8, LANES), 0)
    diag = jnp.zeros((8, LANES), F32)
    for i in range(0, blocks, 2):
        out_ref[0, at:at + LANES] = jnp.where(row <= col, parts[i, i], parts[i + 1, i + 1]).astype(BF16)
        at += LANES
        line = jnp.sum(jnp.where(row == col, parts[i + 1, i + 1], 0.0), axis=0, keepdims=True)
        diag = jnp.where(sub == i // 2, line, diag)
    half = 4
    wide = jnp.zeros((8, LANES), F32)
    for k in range(blocks):
        wide = jnp.where(sub % half == k, rhs[:, k * LANES:(k + 1) * LANES], wide)
    high = wide.astype(BF16).astype(F32)
    wide = jnp.where(sub < half, high, wide - high)
    out_ref[0, at:at + EXTRA] = jnp.concatenate([wide, diag], axis=0).astype(BF16)


def gram_call(obs_ens, weight, innov, order, count, offset, number):
    groups, slots, members = obs_ens.shape
    rows = packed_rows(members)
    return pl.pallas_call(
        functools.partial(gram_kernel, offset),
        out_shape=jax.ShapeDtypeStruct((number, rows, LANES), BF16),
        grid_spec=pltpu.PrefetchScalarGridSpec(
            num_scalar_prefetch=2,
            grid=(number,),
            in_specs=[
                pl.BlockSpec((1, slots, members), lambda i, order, count: (order[offset + i], 0, 0)),
                pl.BlockSpec((groups, slots), lambda i, order, count: (0, 0)),
                pl.BlockSpec((groups, slots), lambda i, order, count: (0, 0)),
            ],
            out_specs=pl.BlockSpec((1, rows, LANES), lambda i, order, count: (i, 0, 0)),
        ),
        cost_estimate=pl.CostEstimate(
            flops=2 * number * slots * members * members, transcendentals=0,
            bytes_accessed=number * 2 * (slots * members + rows * LANES)),
        name="gram",
    )(order, count, obs_ens, weight, innov)


def add_kernel(a_ref, b_ref, out_ref):
    total = a_ref[0].astype(F32) + b_ref[0].astype(F32)
    rows = total.shape[0] - EXTRA
    out_ref[0, :rows] = total[:rows].astype(BF16)
    tail = total[rows:]
    sub = lax.broadcasted_iota(jnp.int32, (8, LANES), 0)
    wide = tail[:8] + pltpu.roll(tail[:8], 4, 0)
    high = wide.astype(BF16).astype(F32)
    wide = jnp.where(sub < 4, high, wide - high)
    out_ref[0, rows:] = jnp.concatenate([wide, tail[8:]], axis=0).astype(BF16)


def add_call(a, b):
    number, rows, lanes = a.shape
    spec = pl.BlockSpec((1, rows, lanes), lambda i: (i, 0, 0))
    return pl.pallas_call(
        add_kernel,
        out_shape=jax.ShapeDtypeStruct(a.shape, a.dtype),
        grid=(number,), in_specs=[spec, spec], out_specs=spec,
        cost_estimate=pl.CostEstimate(flops=a.size, transcendentals=0, bytes_accessed=6 * a.size),
        name="add_parts",
    )(a, b)


def solve_kernel(order_ref, total_ref, state_ref, out_ref):
    members = state_ref.shape[2]
    blocks = members // LANES
    row, col = square_iota()
    grid = {}
    at = 0
    for i, j in block_pairs(blocks):
        part = total_ref[0, at:at + LANES].astype(F32)
        grid[i, j] = part
        grid[j, i] = jnp.transpose(part)
        at += LANES
    base = at + (blocks // 2) * LANES
    tail = total_ref[0, base:base + EXTRA].astype(F32)
    for i in range(0, blocks, 2):
        part = total_ref[0, at:at + LANES].astype(F32)
        flip = jnp.transpose(part)
        at += LANES
        grid[i, i] = jnp.where(row <= col, part, flip)
        low = jnp.where(row > col, part, flip)
        line = tail[8 + i // 2:9 + i // 2]
        grid[i + 1, i + 1] = jnp.where(row == col, line, low)
    gram = jnp.concatenate(
        [jnp.concatenate([grid[i, j] for j in range(blocks)], axis=1) for i in range(blocks)], axis=0)
    big_row = lax.broadcasted_iota(jnp.int32, (members, members), 0)
    big_col = lax.broadcasted_iota(jnp.int32, (members, members), 1)
    eye = big_row == big_col
    matrix = gram + jnp.where(eye, members - 1.0, 0.0)
    square = jnp.sum(matrix * matrix, axis=0, keepdims=True)
    scale = jnp.sqrt(jnp.sum(square, axis=1, keepdims=True))
    root = (matrix / scale).astype(BF16)

    def mul(a, b):
        return jnp.dot(a, b, preferred_element_type=F32)

    inverse = None
    for iteration in range(NS_IT):
        product = root.astype(F32) if inverse is None else mul(inverse, root)
        factor = (jnp.where(eye, 1.5, 0.0) - 0.5 * product).astype(BF16)
        inverse = factor if inverse is None else mul(factor, inverse).astype(BF16)
        if iteration + 1 < NS_IT:
            root = mul(root, factor).astype(BF16)

    sub = lax.broadcasted_iota(jnp.int32, (16, LANES), 0)
    lines = [
        jnp.where(sub == 0, tail[k:k + 1], jnp.where(sub == 1, tail[4 + k:5 + k], 0.0))
        for k in range(blocks)]
    rhs = jnp.concatenate(lines, axis=1).astype(BF16)
    half_way = jnp.sum(mul(rhs, inverse), axis=0, keepdims=True)
    wide = inverse.astype(F32)
    mean_weight = jnp.sum(wide * half_way, axis=1, keepdims=True) / scale
    weights = (jnp.sqrt((members - 1.0) / scale) * wide + mean_weight).astype(BF16)

    state = state_ref[0].astype(F32)
    state_mean = jnp.mean(state, axis=1, keepdims=True)
    state_pert = (state - state_mean).astype(BF16)
    out_ref[0] = (state_mean + mul(state_pert, weights)).astype(BF16)


def solve_call(total, background, order, offset):
    number, rows, lanes = total.shape
    here, members = background.shape[1:]
    return pl.pallas_call(
        solve_kernel,
        out_shape=jax.ShapeDtypeStruct((number, here, members), BF16),
        grid_spec=pltpu.PrefetchScalarGridSpec(
            num_scalar_prefetch=1,
            grid=(number,),
            in_specs=[
                pl.BlockSpec((1, rows, lanes), lambda i, order: (i, 0, 0)),
                pl.BlockSpec((1, here, members), lambda i, order: (order[offset + i], 0, 0)),
            ],
            out_specs=pl.BlockSpec((1, here, members), lambda i, order: (i, 0, 0)),
        ),
        cost_estimate=pl.CostEstimate(
            flops=number * (3 * NS_IT - 3) * 2 * members ** 3, transcendentals=0,
            bytes_accessed=number * (2 * rows * lanes + 4 * here * members)),
        name="solve",
    )(order, total, background)


def pack_rows(array_in, send_index, send_live):
    picked = jnp.take(array_in, send_index, axis=0)
    keep_mask = send_live.reshape((-1,) + (1,) * (array_in.ndim - 1))
    return jnp.where(keep_mask, picked, jnp.zeros_like(picked))


def send_all(result, dest, my_dest, grp_size, grp_index):
    local_groups = result.shape[0]
    group_ids = jnp.arange(dest.shape[0], dtype=jnp.int32)
    same_dest = dest[None, :] == dest[:, None]
    earlier = group_ids[None, :] < group_ids[:, None]
    arrival_rank = jnp.sum(jnp.where(same_dest & earlier, 1, 0), axis=1).astype(jnp.int32)
    peer_ids = jnp.arange(grp_size, dtype=jnp.int32)
    local_ids = jnp.arange(local_groups, dtype=jnp.int32)
    peer_hits = my_dest[None, :] == peer_ids[:, None]
    send_index = jnp.sum(jnp.where(peer_hits, local_ids[None, :], 0), axis=1)
    send_live = jnp.any(peer_hits, axis=1)
    arriving = (dest[None, :] == grp_index) & (arrival_rank[None, :] == local_ids[:, None])
    arrive_group = jnp.sum(jnp.where(arriving, group_ids[None, :], 0), axis=1)
    received = lax.all_to_all(
        pack_rows(result, send_index, send_live), "grp", split_axis=0, concat_axis=0, tiled=True)
    return jnp.take(received, arrive_group // local_groups, axis=0)


def body(background, obs_ens, innovation, obs_weight, obs_count, dest):
    grp_size, own_size = lax.axis_size("grp"), lax.axis_size("own")
    grp_index, own_index = lax.axis_index("grp"), lax.axis_index("own")
    groups = background.shape[0]
    my_dest = lax.dynamic_slice_in_dim(dest, grp_index * groups, groups)
    odd = own_index % 2
    run = groups // 4
    far = list(range(groups - 1, -1, -1))
    head, last = far[:2 * run], far[2 * run:]
    runs = [head[:run], head[run:], last[1::2], last[0::2]]
    runs[2], runs[3] = sorted(runs[2], reverse=True), sorted(runs[3], reverse=True)
    even_seq = runs[0] + runs[1] + runs[2] + runs[3]
    odd_seq = runs[1] + runs[0] + runs[3] + runs[2]
    distance = jnp.where(odd == 1, jnp.array(odd_seq, jnp.int32), jnp.array(even_seq, jnp.int32))
    direct = grp_size == groups and groups & (groups - 1) == 0
    if direct:
        target = grp_index ^ distance
        order = jnp.sum(
            jnp.where(my_dest[None, :] == target[:, None], jnp.arange(groups, dtype=jnp.int32)[None, :], 0),
            axis=1).astype(jnp.int32)
    else:
        order = distance
    count = obs_count[:, 0]

    pair = [(i, i ^ 1) for i in range(own_size)]
    crosses = []
    while 2 << len(crosses) < own_size:
        step = 2 << len(crosses)
        crosses.append([(i, i ^ step) for i in range(own_size)])
    results = []
    for chunk in range(2):
        at = 2 * run * chunk
        send = gram_call(obs_ens, obs_weight, innovation, order, count, at + run, run)
        keep = gram_call(obs_ens, obs_weight, innovation, order, count, at, run)
        mine = add_call(keep, lax.ppermute(send, "own", pair))
        for cross in crosses:
            mine = add_call(mine, lax.ppermute(mine, "own", cross))
        other = lax.ppermute(mine, "own", pair)
        for total, offset in ((mine, at), (other, at + run)):
            done = solve_call(total, background, order, offset)
            results += [done[k:k + 1] for k in range(run)]
    if not direct:
        back = jnp.zeros_like(order).at[order].set(jnp.arange(groups, dtype=jnp.int32))
        result = jnp.take(jnp.concatenate(results, axis=0), back, axis=0)
        return send_all(result, dest, my_dest, grp_size, grp_index)
    out = jnp.zeros(background.shape, background.dtype)
    for slot, done in enumerate(results):
        pairs = []
        for i in range(grp_size):
            for o in range(own_size):
                step = (odd_seq if o % 2 else even_seq)[slot]
                pairs.append((i * own_size + o, (i ^ step) * own_size + o))
        arrived = lax.ppermute(done, ("grp", "own"), pairs)
        out = lax.dynamic_update_slice_in_dim(out, arrived, target[slot], 0)
    return out


def solution(mesh):
    return jax.shard_map(
        body,
        mesh=mesh,
        in_specs=(
            P("grp", "own", None),
            P("grp", "own", None),
            P("grp", "own"),
            P("grp", "own"),
            P("grp", "own"),
            P(),
        ),
        out_specs=P("grp", "own", None),
        check_vma=False,
    )
```

```python
import functools

import jax
import jax.numpy as jnp
from jax import lax
from jax.experimental import pallas as pl
from jax.experimental.pallas import tpu as pltpu
from jax.sharding import PartitionSpec as P


NS_IT = 4
LANES = 128
EXTRA = 16
F32 = jnp.float32
BF16 = jnp.bfloat16


def block_pairs(blocks):
    return [(i, j) for i in range(blocks) for j in range(i + 1, blocks)]


def packed_rows(members):
    blocks = members // LANES
    return (len(block_pairs(blocks)) + blocks // 2) * LANES + EXTRA


def square_iota():
    row = lax.broadcasted_iota(jnp.int32, (LANES, LANES), 0)
    col = lax.broadcasted_iota(jnp.int32, (LANES, LANES), 1)
    return row, col


def store_packed(out_ref, place, blocks, part, tail):
    row, col = square_iota()
    at = 0
    for i, j in block_pairs(blocks):
        out_ref[place, at:at + LANES] = part(i, j).astype(BF16)
        at += LANES
    sub = lax.broadcasted_iota(jnp.int32, (8, LANES), 0)
    low = tail[8:]
    for i in range(0, blocks, 2):
        second = part(i + 1, i + 1)
        out_ref[place, at:at + LANES] = jnp.where(row <= col, part(i, i), second).astype(BF16)
        at += LANES
        line = jnp.sum(jnp.where(row == col, second, 0.0), axis=0, keepdims=True)
        low = jnp.where(sub == i // 2, line, low)
    out_ref[place, at:at + EXTRA] = jnp.concatenate([tail[:8], low], axis=0).astype(BF16)


def load_packed(buf, k, members):
    blocks = members // LANES
    row, col = square_iota()
    base = packed_rows(members) - EXTRA
    tail = buf[k, base:base + EXTRA].astype(F32)
    grid = {}
    at = 0
    for i, j in block_pairs(blocks):
        part = buf[k, at:at + LANES].astype(F32)
        grid[i, j] = part
        grid[j, i] = jnp.transpose(part)
        at += LANES
    for i in range(0, blocks, 2):
        part = buf[k, at:at + LANES].astype(F32)
        flip = jnp.transpose(part)
        at += LANES
        grid[i, i] = jnp.where(row <= col, part, flip)
        low = jnp.where(row > col, part, flip)
        grid[i + 1, i + 1] = jnp.where(row == col, tail[8 + i // 2:9 + i // 2], low)
    whole = jnp.concatenate(
        [jnp.concatenate([grid[i, j] for j in range(blocks)], axis=1) for i in range(blocks)], axis=0)
    return whole, tail


def split_rows(line, blocks):
    sub = lax.broadcasted_iota(jnp.int32, (8, LANES), 0)
    wide = jnp.zeros((8, LANES), F32)
    for i in range(blocks):
        wide = jnp.where(sub % 4 == i, line[:, i * LANES:(i + 1) * LANES], wide)
    high = wide.astype(BF16).astype(F32)
    return jnp.where(sub < 4, high, wide - high)


def pick_group(dest_ref, plan, slot):
    even_seq, odd_seq, groups, direct = plan
    own_index, grp_index = lax.axis_index("own"), lax.axis_index("grp")
    step = jnp.where(own_index % 2 == 1, odd_seq[slot], even_seq[slot])
    if not direct:
        return step
    target = grp_index ^ step
    found = jnp.int32(0)
    for k in range(groups):
        found = found + jnp.where(dest_ref[grp_index * groups + k] == target, k, 0)
    return found


def gram_kernel(plan, wanted, dest_ref, count_ref, obs_ref, weight_ref, innov_ref, *refs):
    out_refs, (obs_buf, sem) = refs[:len(wanted)], refs[len(wanted):]
    number, slots, members = obs_buf.shape
    blocks = members // LANES
    picked = [pick_group(dest_ref, plan, slot) for slots_here in wanted for slot in slots_here]
    places = [(ref, k) for ref, slots_here in zip(out_refs, wanted) for k in range(len(slots_here))]
    copies = [pltpu.make_async_copy(obs_ref.at[g], obs_buf.at[k], sem.at[k]) for k, g in enumerate(picked)]
    for copy in copies:
        copy.start()

    def own_row(ref, group):
        rows = lax.broadcasted_iota(jnp.int32, ref.shape, 0)
        return jnp.sum(jnp.where(rows == group, ref[...].astype(F32), 0.0), axis=0, keepdims=True)

    columns, sources = [], []
    for group in picked:
        live = lax.broadcasted_iota(jnp.int32, (1, slots), 1) < count_ref[group]
        weight = jnp.where(live, own_row(weight_ref, group), 0.0)
        sources.append((weight * own_row(innov_ref, group)).astype(BF16))
        column = jnp.transpose(jnp.broadcast_to(weight, (LANES, slots)))
        columns.append(jnp.concatenate([column] * blocks, axis=1))
    perts, scaled = [], []
    for k in range(number):
        copies[k].wait()
        obs = obs_buf[k].astype(F32)
        mean = jnp.mean(obs, axis=1, keepdims=True)
        pert = (obs - mean).astype(BF16)
        perts.append(pert)
        scaled.append((pert.astype(F32) * columns[k]).astype(BF16))
    for k in range(number):
        pert, weighted = perts[k], scaled[k]
        out_ref, place = places[k]
        parts = {}
        for i in range(0, blocks, 2):
            strip = lax.dot_general(
                weighted[:, i * LANES:(i + 2) * LANES], pert[:, i * LANES:],
                (((0,), (0,)), ((), ())), preferred_element_type=F32)
            for a in range(2):
                for j in range(i + a, blocks):
                    parts[i + a, j] = strip[a * LANES:(a + 1) * LANES, (j - i) * LANES:(j - i + 1) * LANES]
        rhs = jnp.dot(jnp.broadcast_to(sources[k], (16, slots)), pert, preferred_element_type=F32)[:8]
        tail = jnp.concatenate([split_rows(rhs, blocks), jnp.zeros((8, LANES), F32)], axis=0)
        store_packed(out_ref, place, blocks, lambda i, j: parts[i, j], tail)


def gram_call(obs_ens, weight, innov, dest, count, plan, wanted):
    _, slots, members = obs_ens.shape
    rows = packed_rows(members)
    number = sum(len(slots_here) for slots_here in wanted)
    return pl.pallas_call(
        functools.partial(gram_kernel, plan, wanted),
        out_shape=[jax.ShapeDtypeStruct((len(slots_here), rows, LANES), BF16) for slots_here in wanted],
        in_specs=[
            pl.BlockSpec(memory_space=pltpu.SMEM),
            pl.BlockSpec(memory_space=pltpu.SMEM),
            pl.BlockSpec(memory_space=pl.ANY),
            pl.BlockSpec(memory_space=pltpu.VMEM),
            pl.BlockSpec(memory_space=pltpu.VMEM),
        ],
        out_specs=[pl.BlockSpec(memory_space=pltpu.VMEM)] * len(wanted),
        scratch_shapes=[pltpu.VMEM((number, slots, members), BF16), pltpu.SemaphoreType.DMA((number,))],
        cost_estimate=pl.CostEstimate(
            flops=2 * number * slots * members * members, transcendentals=0,
            bytes_accessed=number * 2 * (slots * members + rows * LANES)),
        name="gram",
    )(dest, count, obs_ens, weight, innov)


def add_parts(a, b):
    rows = a.shape[1]
    main = (a.astype(F32) + b.astype(F32)).astype(BF16)
    tail = a[:, rows - EXTRA:rows - 8].astype(F32) + b[:, rows - EXTRA:rows - 8].astype(F32)
    wide = tail[:, :4] + tail[:, 4:]
    high = lax.reduce_precision(wide, 8, 7)
    split = jnp.concatenate([high, wide - high], axis=1).astype(BF16)
    return lax.dynamic_update_slice(main, split, (0, rows - EXTRA, 0))


def apply_rows(state, weights):
    state = state.astype(F32)
    state_mean = jnp.mean(state, axis=1, keepdims=True)
    state_pert = (state - state_mean).astype(BF16)
    return (state_mean + jnp.dot(state_pert, weights, preferred_element_type=F32)).astype(BF16)


def solve_kernel(plan, offset, number, dest_ref, total_ref, state_ref, *refs):
    out_refs, (total_buf, state_buf, sem, state_sem) = refs[:-4], refs[-4:]
    members = state_buf.shape[2]
    blocks = members // LANES
    fetch = [pltpu.make_async_copy(total_ref.at[k], total_buf.at[k], sem.at[k]) for k in range(number)]
    picked = [pick_group(dest_ref, plan, offset + k) for k in range(number)]
    states = [
        pltpu.make_async_copy(state_ref.at[g], state_buf.at[k], state_sem.at[k]) for k, g in enumerate(picked)]
    for copy in fetch + states:
        copy.start()
    big_row = lax.broadcasted_iota(jnp.int32, (members, members), 0)
    big_col = lax.broadcasted_iota(jnp.int32, (members, members), 1)
    eye = big_row == big_col
    sub = lax.broadcasted_iota(jnp.int32, (16, LANES), 0)

    def mul(a, b):
        return jnp.dot(a, b, preferred_element_type=F32)

    roots, scales, rhs = [], [], []
    for k in range(number):
        fetch[k].wait()
        gram, tail = load_packed(total_buf, k, members)
        matrix = gram + jnp.where(eye, members - 1.0, 0.0)
        square = jnp.sum(matrix * matrix, axis=0, keepdims=True)
        scale = jnp.sqrt(jnp.sum(square, axis=1, keepdims=True))
        scales.append(scale)
        roots.append((matrix / scale).astype(BF16))
        lines = [
            jnp.where(sub == 0, tail[i:i + 1], jnp.where(sub == 1, tail[4 + i:5 + i], 0.0))
            for i in range(blocks)]
        rhs.append(jnp.concatenate(lines, axis=1).astype(BF16))

    inverses = [None] * number
    for iteration in range(NS_IT):
        products = [
            root.astype(F32) if inverse is None else mul(inverse, root) for inverse, root in zip(inverses, roots)]
        factors = [(jnp.where(eye, 1.5, 0.0) - 0.5 * product).astype(BF16) for product in products]
        inverses = [
            factor if inverse is None else mul(factor, inverse).astype(BF16)
            for inverse, factor in zip(inverses, factors)]
        if iteration + 1 < NS_IT:
            roots = [mul(root, factor).astype(BF16) for root, factor in zip(roots, factors)]

    for k in range(number):
        half_way = jnp.sum(mul(rhs[k], inverses[k]), axis=0, keepdims=True)
        wide = inverses[k].astype(F32)
        mean_weight = jnp.sum(wide * half_way, axis=1, keepdims=True) / scales[k]
        spread = jnp.sqrt((members - 1.0) / scales[k])
        if len(out_refs) > number:
            flat = jnp.transpose(jnp.broadcast_to(mean_weight, (members, LANES)))[:1]
            tail = jnp.zeros((8, LANES), F32)
            left = jnp.broadcast_to(spread, (8, LANES))
            for place in range(4, 7):
                term = left.astype(BF16).astype(F32)
                tail = jnp.where(sub[:8] == place, term, tail)
                left = left - term
            tail = jnp.concatenate([split_rows(flat, blocks), tail], axis=0)
            store_packed(
                out_refs[number], k, blocks,
                lambda i, j: wide[i * LANES:(i + 1) * LANES, j * LANES:(j + 1) * LANES], tail)
        weights = (spread * wide + mean_weight).astype(BF16)
        states[k].wait()
        out_refs[k][0] = apply_rows(state_buf[k], weights)


def apply_kernel(plan, offset, number, dest_ref, packed_ref, state_ref, *refs):
    out_refs, (packed_buf, state_buf, sem, state_sem) = refs[:-4], refs[-4:]
    members = state_buf.shape[2]
    blocks = members // LANES
    fetch = [pltpu.make_async_copy(packed_ref.at[k], packed_buf.at[k], sem.at[k]) for k in range(number)]
    picked = [pick_group(dest_ref, plan, offset + k) for k in range(number)]
    states = [
        pltpu.make_async_copy(state_ref.at[g], state_buf.at[k], state_sem.at[k]) for k, g in enumerate(picked)]
    for copy in fetch + states:
        copy.start()
    for k in range(number):
        fetch[k].wait()
        inverse, tail = load_packed(packed_buf, k, members)
        spread = tail[12:13, :1] + tail[13:14, :1] + tail[14:15, :1]
        means = tail[:8] + pltpu.roll(tail[:8], 4, 0)
        column = jnp.concatenate(
            [jnp.transpose(jnp.broadcast_to(means[i:i + 1], (LANES, LANES))) for i in range(blocks)], axis=0)
        column = jnp.concatenate([column] * blocks, axis=1)
        weights = (spread * inverse + column).astype(BF16)
        states[k].wait()
        out_refs[k][0] = apply_rows(state_buf[k], weights)


def solve_call(total, background, dest, plan, offset, kernel, emit):
    number, rows, lanes = total.shape
    here, members = background.shape[1:]
    products = 3 * NS_IT - 3 if kernel is solve_kernel else 1
    packed = [jax.ShapeDtypeStruct((number, rows, lanes), BF16)] if emit else []
    return pl.pallas_call(
        functools.partial(kernel, plan, offset, number),
        out_shape=[jax.ShapeDtypeStruct((1, here, members), BF16)] * number + packed,
        in_specs=[
            pl.BlockSpec(memory_space=pltpu.SMEM),
            pl.BlockSpec(memory_space=pl.ANY),
            pl.BlockSpec(memory_space=pl.ANY),
        ],
        out_specs=[pl.BlockSpec(memory_space=pltpu.VMEM)] * (number + len(packed)),
        scratch_shapes=[
            pltpu.VMEM((number, rows, lanes), BF16), pltpu.VMEM((number, here, members), BF16),
            pltpu.SemaphoreType.DMA((number,)), pltpu.SemaphoreType.DMA((number,))],
        cost_estimate=pl.CostEstimate(
            flops=number * products * 2 * members ** 3, transcendentals=0,
            bytes_accessed=number * (2 * rows * lanes + 4 * here * members)),
        name="solve" if kernel is solve_kernel else "apply",
    )(dest, total, background)


def pack_rows(array_in, send_index, send_live):
    picked = jnp.take(array_in, send_index, axis=0)
    keep_mask = send_live.reshape((-1,) + (1,) * (array_in.ndim - 1))
    return jnp.where(keep_mask, picked, jnp.zeros_like(picked))


def send_all(result, dest, my_dest, grp_size, grp_index):
    local_groups = result.shape[0]
    group_ids = jnp.arange(dest.shape[0], dtype=jnp.int32)
    same_dest = dest[None, :] == dest[:, None]
    earlier = group_ids[None, :] < group_ids[:, None]
    arrival_rank = jnp.sum(jnp.where(same_dest & earlier, 1, 0), axis=1).astype(jnp.int32)
    peer_ids = jnp.arange(grp_size, dtype=jnp.int32)
    local_ids = jnp.arange(local_groups, dtype=jnp.int32)
    peer_hits = my_dest[None, :] == peer_ids[:, None]
    send_index = jnp.sum(jnp.where(peer_hits, local_ids[None, :], 0), axis=1)
    send_live = jnp.any(peer_hits, axis=1)
    arriving = (dest[None, :] == grp_index) & (arrival_rank[None, :] == local_ids[:, None])
    arrive_group = jnp.sum(jnp.where(arriving, group_ids[None, :], 0), axis=1)
    received = lax.all_to_all(
        pack_rows(result, send_index, send_live), "grp", split_axis=0, concat_axis=0, tiled=True)
    return jnp.take(received, arrive_group // local_groups, axis=0)


def body(background, obs_ens, innovation, obs_weight, obs_count, dest):
    grp_size, own_size = lax.axis_size("grp"), lax.axis_size("own")
    grp_index, own_index = lax.axis_index("grp"), lax.axis_index("own")
    groups = background.shape[0]
    odd = own_index % 2
    quarter = groups // 8
    sizes = [quarter, groups // 2 - 2 * quarter, quarter]
    even_seq, odd_seq, slots, at = [], [], [], 0
    far = list(range(groups - 1, -1, -1))
    for size in sizes:
        block = far[2 * at:2 * (at + size)]
        even_seq += block[0::2] + block[1::2]
        odd_seq += block[1::2] + block[0::2]
        slots.append((tuple(range(2 * at, 2 * at + size)), tuple(range(2 * at + size, 2 * (at + size)))))
        at += size
    direct = grp_size == groups and groups & (groups - 1) == 0
    plan = (tuple(even_seq), tuple(odd_seq), groups, direct)

    count = obs_count.reshape(groups)
    pair = [(i, i ^ 1) for i in range(own_size)]
    crosses = []
    while 2 << len(crosses) < own_size:
        step = 2 << len(crosses)
        crosses.append([(i, i ^ step) for i in range(own_size)])

    def gram(wanted):
        return gram_call(obs_ens, obs_weight, innovation, dest, count, plan, wanted)

    sends, keeps = [None] * 3, [None] * 3
    sends[0], = gram((slots[0][1],))
    keeps[0], sends[1] = gram((slots[0][0], slots[1][1]))
    keeps[1], sends[2], keeps[2] = gram((slots[1][0], slots[2][1], slots[2][0]))
    results = [None] * groups
    for chunk, (kept, given) in enumerate(slots):
        arrived = lax.ppermute(sends[chunk], "own", pair)
        mine = add_parts(keeps[chunk], arrived)
        for cross in crosses:
            arrived = lax.ppermute(mine, "own", cross)
            mine = add_parts(mine, arrived)
        last = chunk == 2
        if last:
            other = lax.ppermute(mine, "own", pair)
        solved = solve_call(mine, background, dest, plan, kept[0], solve_kernel, not last)
        if not last:
            other = lax.ppermute(solved[-1], "own", pair)
        results[kept[0]:kept[0] + len(kept)] = solved[:len(kept)]
        results[given[0]:given[0] + len(given)] = solve_call(
            other, background, dest, plan, given[0], solve_kernel if last else apply_kernel, False)
    if not direct:
        even_back, odd_back = ([seq.index(k) for k in range(groups)] for seq in (even_seq, odd_seq))
        back = jnp.where(odd == 1, jnp.array(odd_back, jnp.int32), jnp.array(even_back, jnp.int32))
        result = jnp.take(jnp.concatenate(results, axis=0), back, axis=0)
        my_dest = lax.dynamic_slice_in_dim(dest, grp_index * groups, groups)
        return send_all(result, dest, my_dest, grp_size, grp_index)
    out = jnp.zeros(background.shape, background.dtype)
    arrivals, sources = [], []
    for slot, done in enumerate(results):
        pairs = []
        for i in range(grp_size):
            for o in range(own_size):
                step = (odd_seq if o % 2 else even_seq)[slot]
                pairs.append((i * own_size + o, (i ^ step) * own_size + o))
        arrivals.append(lax.ppermute(done, ("grp", "own"), pairs))
        sources.append(grp_index ^ jnp.where(odd == 1, odd_seq[slot], even_seq[slot]))
    late, _ = lax.optimization_barrier((tuple(arrivals[:-1]), results[-1]))
    for arrived, source in zip(late + (arrivals[-1],), sources):
        out = lax.dynamic_update_slice_in_dim(out, arrived, source, 0)
    return out


def solution(mesh):
    return mapped(mesh)


def mapped(mesh):
    return jax.shard_map(
        body,
        mesh=mesh,
        in_specs=(
            P("grp", "own", None),
            P("grp", "own", None),
            P("grp", "own"),
            P("grp", "own"),
            P("grp", "own"),
            P(),
        ),
        out_specs=P("grp", "own", None),
        check_vma=False,
    )
```

```python
import functools

import jax
import jax.numpy as jnp
from jax import lax
from jax.experimental import pallas as pl
from jax.experimental.pallas import tpu as pltpu
from jax.sharding import PartitionSpec as P


NS_IT = 4
LANES = 128
EXTRA = 16
F32 = jnp.float32
BF16 = jnp.bfloat16


def block_pairs(blocks):
    return [(i, j) for i in range(blocks) for j in range(i + 1, blocks)]


def packed_rows(members):
    blocks = members // LANES
    return (len(block_pairs(blocks)) + blocks // 2) * LANES + EXTRA


def square_iota():
    row = lax.broadcasted_iota(jnp.int32, (LANES, LANES), 0)
    col = lax.broadcasted_iota(jnp.int32, (LANES, LANES), 1)
    return row, col


def store_packed(out_ref, place, blocks, part, tail):
    row, col = square_iota()
    at = 0
    for i, j in block_pairs(blocks):
        out_ref[place, at:at + LANES] = part(i, j).astype(BF16)
        at += LANES
    sub = lax.broadcasted_iota(jnp.int32, (8, LANES), 0)
    low = tail[8:]
    for i in range(0, blocks, 2):
        second = part(i + 1, i + 1)
        out_ref[place, at:at + LANES] = jnp.where(row <= col, part(i, i), second).astype(BF16)
        at += LANES
        line = jnp.sum(jnp.where(row == col, second, 0.0), axis=0, keepdims=True)
        low = jnp.where(sub == i // 2, line, low)
    out_ref[place, at:at + EXTRA] = jnp.concatenate([tail[:8], low], axis=0).astype(BF16)


def load_packed(buf, k, members):
    blocks = members // LANES
    row, col = square_iota()
    base = packed_rows(members) - EXTRA
    tail = buf[k, base:base + EXTRA].astype(F32)
    grid = {}
    at = 0
    for i, j in block_pairs(blocks):
        part = buf[k, at:at + LANES].astype(F32)
        grid[i, j] = part
        grid[j, i] = jnp.transpose(part)
        at += LANES
    for i in range(0, blocks, 2):
        part = buf[k, at:at + LANES].astype(F32)
        flip = jnp.transpose(part)
        at += LANES
        grid[i, i] = jnp.where(row <= col, part, flip)
        low = jnp.where(row > col, part, flip)
        grid[i + 1, i + 1] = jnp.where(row == col, tail[8 + i // 2:9 + i // 2], low)
    whole = jnp.concatenate(
        [jnp.concatenate([grid[i, j] for j in range(blocks)], axis=1) for i in range(blocks)], axis=0)
    return whole, tail


def split_rows(line, blocks):
    sub = lax.broadcasted_iota(jnp.int32, (8, LANES), 0)
    wide = jnp.zeros((8, LANES), F32)
    for i in range(blocks):
        wide = jnp.where(sub % 4 == i, line[:, i * LANES:(i + 1) * LANES], wide)
    high = wide.astype(BF16).astype(F32)
    return jnp.where(sub < 4, high, wide - high)


def pick_group(dest_ref, plan, slot):
    even_seq, odd_seq, groups, direct = plan
    own_index, grp_index = lax.axis_index("own"), lax.axis_index("grp")
    step = jnp.where(own_index % 2 == 1, odd_seq[slot], even_seq[slot])
    if not direct:
        return step
    target = grp_index ^ step
    found = jnp.int32(0)
    for k in range(groups):
        found = found + jnp.where(dest_ref[grp_index * groups + k] == target, k, 0)
    return found


def gram_kernel(plan, wanted, dest_ref, count_ref, obs_ref, weight_ref, innov_ref, *refs):
    out_refs, (obs_buf, sem) = refs[:len(wanted)], refs[len(wanted):]
    number, slots, members = obs_buf.shape
    blocks = members // LANES
    picked = [pick_group(dest_ref, plan, slot) for slots_here in wanted for slot in slots_here]
    places = [(ref, k) for ref, slots_here in zip(out_refs, wanted) for k in range(len(slots_here))]
    copies = [pltpu.make_async_copy(obs_ref.at[g], obs_buf.at[k], sem.at[k]) for k, g in enumerate(picked)]
    for copy in copies:
        copy.start()

    def own_row(ref, group):
        rows = lax.broadcasted_iota(jnp.int32, ref.shape, 0)
        return jnp.sum(jnp.where(rows == group, ref[...].astype(F32), 0.0), axis=0, keepdims=True)

    columns, sources = [], []
    for group in picked:
        live = lax.broadcasted_iota(jnp.int32, (1, slots), 1) < count_ref[group]
        weight = jnp.where(live, own_row(weight_ref, group), 0.0)
        sources.append((weight * own_row(innov_ref, group)).astype(BF16))
        column = jnp.transpose(jnp.broadcast_to(weight, (LANES, slots)))
        columns.append(jnp.concatenate([column] * blocks, axis=1))
    perts, scaled = [], []
    for k in range(number):
        copies[k].wait()
        obs = obs_buf[k].astype(F32)
        mean = jnp.mean(obs, axis=1, keepdims=True)
        pert = (obs - mean).astype(BF16)
        perts.append(pert)
        scaled.append((pert.astype(F32) * columns[k]).astype(BF16))
    for k in range(number):
        pert, weighted = perts[k], scaled[k]
        out_ref, place = places[k]
        parts = {}
        for i in range(0, blocks, 2):
            strip = lax.dot_general(
                weighted[:, i * LANES:(i + 2) * LANES], pert[:, i * LANES:],
                (((0,), (0,)), ((), ())), preferred_element_type=F32)
            for a in range(2):
                for j in range(i + a, blocks):
                    parts[i + a, j] = strip[a * LANES:(a + 1) * LANES, (j - i) * LANES:(j - i + 1) * LANES]
        rhs = jnp.dot(jnp.broadcast_to(sources[k], (16, slots)), pert, preferred_element_type=F32)[:8]
        tail = jnp.concatenate([split_rows(rhs, blocks), jnp.zeros((8, LANES), F32)], axis=0)
        store_packed(out_ref, place, blocks, lambda i, j: parts[i, j], tail)


def gram_call(obs_ens, weight, innov, dest, count, plan, wanted):
    _, slots, members = obs_ens.shape
    rows = packed_rows(members)
    number = sum(len(slots_here) for slots_here in wanted)
    return pl.pallas_call(
        functools.partial(gram_kernel, plan, wanted),
        out_shape=[jax.ShapeDtypeStruct((len(slots_here), rows, LANES), BF16) for slots_here in wanted],
        in_specs=[
            pl.BlockSpec(memory_space=pltpu.SMEM),
            pl.BlockSpec(memory_space=pltpu.SMEM),
            pl.BlockSpec(memory_space=pl.ANY),
            pl.BlockSpec(memory_space=pltpu.VMEM),
            pl.BlockSpec(memory_space=pltpu.VMEM),
        ],
        out_specs=[pl.BlockSpec(memory_space=pltpu.VMEM)] * len(wanted),
        scratch_shapes=[pltpu.VMEM((number, slots, members), BF16), pltpu.SemaphoreType.DMA((number,))],
        cost_estimate=pl.CostEstimate(
            flops=2 * number * slots * members * members, transcendentals=0,
            bytes_accessed=number * 2 * (slots * members + rows * LANES)),
        name="gram",
    )(dest, count, obs_ens, weight, innov)


def add_parts(a, b):
    rows = a.shape[1]
    main = (a.astype(F32) + b.astype(F32)).astype(BF16)
    tail = a[:, rows - EXTRA:rows - 8].astype(F32) + b[:, rows - EXTRA:rows - 8].astype(F32)
    wide = tail[:, :4] + tail[:, 4:]
    high = lax.reduce_precision(wide, 8, 7)
    split = jnp.concatenate([high, wide - high], axis=1).astype(BF16)
    return lax.dynamic_update_slice(main, split, (0, rows - EXTRA, 0))


def apply_rows(state, weights):
    state = state.astype(F32)
    state_mean = jnp.mean(state, axis=1, keepdims=True)
    state_pert = (state - state_mean).astype(BF16)
    return (state_mean + jnp.dot(state_pert, weights, preferred_element_type=F32)).astype(BF16)


def solve_kernel(plan, offset, number, dest_ref, total_ref, state_ref, *refs):
    out_refs, (state_buf, state_sem) = refs[:-2], refs[-2:]
    members = state_buf.shape[2]
    blocks = members // LANES
    picked = [pick_group(dest_ref, plan, offset + k) for k in range(number)]
    states = [
        pltpu.make_async_copy(state_ref.at[g], state_buf.at[k], state_sem.at[k]) for k, g in enumerate(picked)]
    for copy in states:
        copy.start()
    big_row = lax.broadcasted_iota(jnp.int32, (members, members), 0)
    big_col = lax.broadcasted_iota(jnp.int32, (members, members), 1)
    eye = big_row == big_col
    sub = lax.broadcasted_iota(jnp.int32, (16, LANES), 0)

    def mul(a, b):
        return jnp.dot(a, b, preferred_element_type=F32)

    roots, scales, rhs = [], [], []
    for k in range(number):
        gram, tail = load_packed(total_ref, k, members)
        matrix = gram + jnp.where(eye, members - 1.0, 0.0)
        square = jnp.sum(matrix * matrix, axis=0, keepdims=True)
        scale = jnp.sqrt(jnp.sum(square, axis=1, keepdims=True))
        scales.append(scale)
        roots.append((matrix / scale).astype(BF16))
        lines = [
            jnp.where(sub == 0, tail[i:i + 1], jnp.where(sub == 1, tail[4 + i:5 + i], 0.0))
            for i in range(blocks)]
        rhs.append(jnp.concatenate(lines, axis=1).astype(BF16))

    inverses = [None] * number
    for iteration in range(NS_IT):
        products = [
            root.astype(F32) if inverse is None else mul(inverse, root) for inverse, root in zip(inverses, roots)]
        factors = [(jnp.where(eye, 1.5, 0.0) - 0.5 * product).astype(BF16) for product in products]
        inverses = [
            factor if inverse is None else mul(factor, inverse).astype(BF16)
            for inverse, factor in zip(inverses, factors)]
        if iteration + 1 < NS_IT:
            roots = [mul(root, factor).astype(BF16) for root, factor in zip(roots, factors)]

    for k in range(number):
        half_way = jnp.sum(mul(rhs[k], inverses[k]), axis=0, keepdims=True)
        wide = inverses[k].astype(F32)
        mean_weight = jnp.sum(wide * half_way, axis=1, keepdims=True) / scales[k]
        spread = jnp.sqrt((members - 1.0) / scales[k])
        if len(out_refs) > number:
            flat = jnp.transpose(jnp.broadcast_to(mean_weight, (members, LANES)))[:1]
            tail = jnp.zeros((8, LANES), F32)
            left = jnp.broadcast_to(spread, (8, LANES))
            for place in range(4, 7):
                term = left.astype(BF16).astype(F32)
                tail = jnp.where(sub[:8] == place, term, tail)
                left = left - term
            tail = jnp.concatenate([split_rows(flat, blocks), tail], axis=0)
            store_packed(
                out_refs[number], k, blocks,
                lambda i, j: wide[i * LANES:(i + 1) * LANES, j * LANES:(j + 1) * LANES], tail)
        weights = (spread * wide + mean_weight).astype(BF16)
        states[k].wait()
        out_refs[k][0] = apply_rows(state_buf[k], weights)


def apply_kernel(plan, offset, number, dest_ref, packed_ref, state_ref, *refs):
    out_refs, (state_buf, state_sem) = refs[:-2], refs[-2:]
    members = state_buf.shape[2]
    blocks = members // LANES
    picked = [pick_group(dest_ref, plan, offset + k) for k in range(number)]
    states = [
        pltpu.make_async_copy(state_ref.at[g], state_buf.at[k], state_sem.at[k]) for k, g in enumerate(picked)]
    for copy in states:
        copy.start()
    for k in range(number):
        inverse, tail = load_packed(packed_ref, k, members)
        spread = tail[12:13, :1] + tail[13:14, :1] + tail[14:15, :1]
        means = tail[:8] + pltpu.roll(tail[:8], 4, 0)
        column = jnp.concatenate(
            [jnp.transpose(jnp.broadcast_to(means[i:i + 1], (LANES, LANES))) for i in range(blocks)], axis=0)
        column = jnp.concatenate([column] * blocks, axis=1)
        weights = (spread * inverse + column).astype(BF16)
        states[k].wait()
        out_refs[k][0] = apply_rows(state_buf[k], weights)


def solve_call(total, background, dest, plan, offset, kernel, emit):
    number, rows, lanes = total.shape
    here, members = background.shape[1:]
    products = 3 * NS_IT - 3 if kernel is solve_kernel else 1
    packed = [jax.ShapeDtypeStruct((number, rows, lanes), BF16)] if emit else []
    return pl.pallas_call(
        functools.partial(kernel, plan, offset, number),
        out_shape=[jax.ShapeDtypeStruct((1, here, members), BF16)] * number + packed,
        in_specs=[
            pl.BlockSpec(memory_space=pltpu.SMEM),
            pl.BlockSpec(memory_space=pltpu.VMEM),
            pl.BlockSpec(memory_space=pl.ANY),
        ],
        out_specs=[pl.BlockSpec(memory_space=pltpu.VMEM)] * (number + len(packed)),
        scratch_shapes=[
            pltpu.VMEM((number, here, members), BF16), pltpu.SemaphoreType.DMA((number,))],
        cost_estimate=pl.CostEstimate(
            flops=number * products * 2 * members ** 3, transcendentals=0,
            bytes_accessed=number * (2 * rows * lanes + 4 * here * members)),
        name="solve" if kernel is solve_kernel else "apply",
    )(dest, total, background)


def pack_rows(array_in, send_index, send_live):
    picked = jnp.take(array_in, send_index, axis=0)
    keep_mask = send_live.reshape((-1,) + (1,) * (array_in.ndim - 1))
    return jnp.where(keep_mask, picked, jnp.zeros_like(picked))


def send_all(result, dest, my_dest, grp_size, grp_index):
    local_groups = result.shape[0]
    group_ids = jnp.arange(dest.shape[0], dtype=jnp.int32)
    same_dest = dest[None, :] == dest[:, None]
    earlier = group_ids[None, :] < group_ids[:, None]
    arrival_rank = jnp.sum(jnp.where(same_dest & earlier, 1, 0), axis=1).astype(jnp.int32)
    peer_ids = jnp.arange(grp_size, dtype=jnp.int32)
    local_ids = jnp.arange(local_groups, dtype=jnp.int32)
    peer_hits = my_dest[None, :] == peer_ids[:, None]
    send_index = jnp.sum(jnp.where(peer_hits, local_ids[None, :], 0), axis=1)
    send_live = jnp.any(peer_hits, axis=1)
    arriving = (dest[None, :] == grp_index) & (arrival_rank[None, :] == local_ids[:, None])
    arrive_group = jnp.sum(jnp.where(arriving, group_ids[None, :], 0), axis=1)
    received = lax.all_to_all(
        pack_rows(result, send_index, send_live), "grp", split_axis=0, concat_axis=0, tiled=True)
    return jnp.take(received, arrive_group // local_groups, axis=0)


def body(background, obs_ens, innovation, obs_weight, obs_count, dest):
    grp_size, own_size = lax.axis_size("grp"), lax.axis_size("own")
    grp_index, own_index = lax.axis_index("grp"), lax.axis_index("own")
    groups = background.shape[0]
    odd = own_index % 2
    quarter = groups // 8
    sizes = [quarter, groups // 2 - 2 * quarter, quarter]
    even_seq, odd_seq, slots, at = [], [], [], 0
    far = list(range(groups - 1, -1, -1))
    for size in sizes:
        block = far[2 * at:2 * (at + size)]
        even_seq += block[0::2] + block[1::2]
        odd_seq += block[1::2] + block[0::2]
        slots.append((tuple(range(2 * at, 2 * at + size)), tuple(range(2 * at + size, 2 * (at + size)))))
        at += size
    direct = grp_size == groups and groups & (groups - 1) == 0
    plan = (tuple(even_seq), tuple(odd_seq), groups, direct)

    count = obs_count.reshape(groups)
    pair = [(i, i ^ 1) for i in range(own_size)]
    crosses = []
    while 2 << len(crosses) < own_size:
        step = 2 << len(crosses)
        crosses.append([(i, i ^ step) for i in range(own_size)])

    def gram(wanted):
        return gram_call(obs_ens, obs_weight, innovation, dest, count, plan, wanted)

    sends, keeps = [None] * 3, [None] * 3
    sends[0], = gram((slots[0][1],))
    keeps[0], sends[1] = gram((slots[0][0], slots[1][1]))
    keeps[1], sends[2], keeps[2] = gram((slots[1][0], slots[2][1], slots[2][0]))
    results = [None] * groups
    for chunk, (kept, given) in enumerate(slots):
        arrived = lax.ppermute(sends[chunk], "own", pair)
        mine = add_parts(keeps[chunk], arrived)
        for cross in crosses:
            arrived = lax.ppermute(mine, "own", cross)
            mine = add_parts(mine, arrived)
        last = chunk == 2
        if last:
            other = lax.ppermute(mine, "own", pair)
        solved = solve_call(mine, background, dest, plan, kept[0], solve_kernel, not last)
        if not last:
            other = lax.ppermute(solved[-1], "own", pair)
        results[kept[0]:kept[0] + len(kept)] = solved[:len(kept)]
        results[given[0]:given[0] + len(given)] = solve_call(
            other, background, dest, plan, given[0], solve_kernel if last else apply_kernel, False)
    if not direct:
        even_back, odd_back = ([seq.index(k) for k in range(groups)] for seq in (even_seq, odd_seq))
        back = jnp.where(odd == 1, jnp.array(odd_back, jnp.int32), jnp.array(even_back, jnp.int32))
        result = jnp.take(jnp.concatenate(results, axis=0), back, axis=0)
        my_dest = lax.dynamic_slice_in_dim(dest, grp_index * groups, groups)
        return send_all(result, dest, my_dest, grp_size, grp_index)
    out = jnp.zeros(background.shape, background.dtype)
    arrivals, sources = [], []
    for slot, done in enumerate(results):
        pairs = []
        for i in range(grp_size):
            for o in range(own_size):
                step = (odd_seq if o % 2 else even_seq)[slot]
                pairs.append((i * own_size + o, (i ^ step) * own_size + o))
        arrivals.append(lax.ppermute(done, ("grp", "own"), pairs))
        sources.append(grp_index ^ jnp.where(odd == 1, odd_seq[slot], even_seq[slot]))
    late, _ = lax.optimization_barrier((tuple(arrivals[:-1]), results[-1]))
    for arrived, source in zip(late + (arrivals[-1],), sources):
        out = lax.dynamic_update_slice_in_dim(out, arrived, source, 0)
    return out


def solution(mesh):
    return mapped(mesh)


def mapped(mesh):
    return jax.shard_map(
        body,
        mesh=mesh,
        in_specs=(
            P("grp", "own", None),
            P("grp", "own", None),
            P("grp", "own"),
            P("grp", "own"),
            P("grp", "own"),
            P(),
        ),
        out_specs=P("grp", "own", None),
        check_vma=False,
    )
```
